512 devices in a mesh: gx: 4 (over y_hi, core), gy: 16 (over z), gz: 8 (over y_lo, x).
Axes of the slice: x: 4, y: 4 (y_hi: 2, y_lo: 2; y = y_hi * 2 + y_lo), z: 16, core: 2. Of those that a mesh axis runs over, the one named last changes fastest.
Arguments:
- heat_level_grid: float32 [256, 1024, 512], P('gz', 'gy', 'gx'), may hold values from -16 to 16, as said below
- interval_first_class: int32 [1], replicated, may hold values from 0 to 95
- interval_beyond_class: int32 [1], replicated, may hold values from 128 to 256
Outputs:
- magnitude: float32 [256, 1024, 512], P('gz', 'gy', 'gx')
- histogram: float32 [256], replicated
- stats: float32 [4], replicated
The draws below stay inside these ranges and needn't reach their ends.
Inputs may be any that keep to these rules, and one draw needn't show every extreme that they name: `heat_level_grid`: each entry is a rough value times an amplitude that is constant on blocks of 8 x 4 x 4 cells (z, y, x) and varies over a factor of 16 between blocks.
All inputs are finite; a program needn't handle non-finite values.
Results may differ from the reference program's by a relative error of at most 0.0003.
Values sent between devices are 32-bit elements; how exact they have to be, the bound alone decides.
A program may use at most 64 MiB of HBM per device.

```python
import math
import jax
import jax.numpy as jnp

BINS = 256
NX = 512
NY = 1024
NZ = 256


def draw_heat_level_grid(key, part):
    first_key, second_key = jax.random.split(jax.random.fold_in(key, 11))
    coarse = jax.random.uniform(first_key, (NZ // 8, NY // 4, NX // 4), jnp.float32, math.log(0.25), math.log(4.0))
    amplitude = jnp.exp(coarse)
    amplitude = jnp.repeat(jnp.repeat(jnp.repeat(amplitude, 8, axis=0), 4, axis=1), 4, axis=2)
    noise = jnp.clip(jax.random.normal(second_key, (NZ, NY, NX), jnp.float32), -4.0, 4.0)
    return (amplitude * noise).astype(jnp.float32)


def setup_inputs(seed: int = 0) -> dict:
    key_list = jax.random.split(jax.random.key(seed), 4)
    return {
        "heat_level_grid": draw_heat_level_grid(jax.random.fold_in(key_list[3], 71), 0),
        "interval_first_class": jax.random.randint(key_list[1], (1,), 0, 96).astype(jnp.int32),
        "interval_beyond_class": jax.random.randint(key_list[2], (1,), 128, BINS + 1).astype(jnp.int32),
    }


stencil_coefficients = (0.8, -0.2, 4.0 / 105.0, -1.0 / 280.0)
grad_range = 12.0

def directional_rate(field, direction_length_count):
    running = jnp.zeros_like(field)
    for offset, coefficient in enumerate(stencil_coefficients, start=1):
        running = running + coefficient * (jnp.roll(field, -offset, direction_length_count) - jnp.roll(field, offset, direction_length_count))
    return running

def reference(heat_level_grid, interval_first_class, interval_beyond_class):
    slope_norm_square = jnp.zeros_like(heat_level_grid)
    for direction_length_count in range(3):
        slope_in_direction = directional_rate(heat_level_grid, direction_length_count)
        slope_norm_square = slope_norm_square + slope_in_direction * slope_in_direction
    magnitude = jnp.sqrt(slope_norm_square + 1.0) - 1.0
    position = jnp.clip(magnitude * (BINS / grad_range), 0.5, BINS - 0.5)
    low_bin = jnp.minimum(jnp.floor(position - 0.5), BINS - 2).astype(jnp.int32)
    fraction = position - 0.5 - low_bin.astype(position.dtype)
    flat_low = low_bin.ravel()
    flat_frac = fraction.ravel()
    counts = jax.ops.segment_sum(1.0 - flat_frac, flat_low, BINS) + jax.ops.segment_sum(flat_frac, flat_low + 1, BINS)
    total_cells = NX * NY * NZ
    histogram = counts * (BINS / total_cells)
    lower_edge = interval_first_class[0]
    upper_edge = interval_beyond_class[0]
    high_bin = low_bin + 1
    inside_low = (low_bin >= lower_edge) & (low_bin < upper_edge)
    inside_high = (high_bin >= lower_edge) & (high_bin < upper_edge)
    weight = jnp.where(inside_low, 1.0 - fraction, 0.0) + jnp.where(inside_high, fraction, 0.0)
    lowest = jnp.min(magnitude + grad_range * (1.0 - weight))
    highest = jnp.max(weight * magnitude)
    weighted_sum = jnp.sum(weight * magnitude) / total_cells
    weighted_count = jnp.sum(weight) / total_cells
    stats = jnp.stack([lowest, highest, weighted_sum, weighted_count])
    return (magnitude, histogram, stats)
```

```python
import jax
import jax.numpy as jnp
from jax import lax
from jax.experimental import pallas as pl
from jax.experimental.pallas import tpu as pltpu
from jax.sharding import PartitionSpec as P

BINS = 256
RANGE = 12.0
COEF = (0.8, -0.2, 4.0 / 105.0, -1.0 / 280.0)
FINE = 11
COARSE = 24
COLS = FINE + 1
MESH = pl.DeviceIdType.MESH
BF = jnp.bfloat16
F32 = jnp.float32


def iota(shape, dim):
    return lax.broadcasted_iota(jnp.int32, shape, dim)


def kernel(nx, ny, nz, cells, first_ref, beyond_ref, x_ref, mag_ref, hist_ref, stat_ref,
           xe, xp, xl, xr, corr, mag, acc, own, plane, line,
           in_sem, out_sem, halo_send, halo_recv, plane_send, plane_recv, line_send, line_recv):
    gx, gy, gz = lax.axis_index("gx"), lax.axis_index("gy"), lax.axis_index("gz")
    zs, ys, lanes = x_ref.shape
    tiles = ys // 8

    load = pltpu.make_async_copy(x_ref, xe.at[pl.ds(4, zs), pl.ds(8, ys), :], in_sem)
    load.start()

    plane_peers = [
        {"gx": lax.rem(gx + dx, nx), "gz": lax.rem(gz + dz, nz)}
        for dx in range(nx) for dz in range(nz) if dx or dz
    ]
    line_peers = [{"gy": lax.rem(gy + d, ny)} for d in range(1, ny)]
    barrier = pltpu.get_barrier_semaphore()
    for peer in plane_peers + line_peers:
        pl.semaphore_signal(barrier, inc=1, device_id=peer, device_id_type=MESH)
    load.wait()

    lane = iota((8, lanes), 1)
    for_group = lane // 8
    part = lane % 8

    def pack(p, carry):
        packed = jnp.zeros((8, lanes), F32)
        for g in range(16):
            tile = xe[4 + 2 * p + g // 8, pl.ds(8 + 8 * (g % 8), 8), :]
            packed = jnp.where(for_group == g, pltpu.roll(tile, (4 + 8 * g) % lanes, 1), packed)
        xp[p] = packed
        return carry

    lax.fori_loop(0, zs // 2, pack, 0)
    acc[...] = jnp.zeros_like(acc)
    pl.semaphore_wait(barrier, len(plane_peers) + len(line_peers))

    def send(i, src, dst, peer):
        copy = pltpu.make_async_remote_copy(
            src_ref=src, dst_ref=dst, send_sem=halo_send.at[i], recv_sem=halo_recv.at[i],
            device_id=peer, device_id_type=MESH)
        copy.start()
        return copy

    up = {"gz": lax.rem(gz + 1, nz)}
    down = {"gz": lax.rem(gz + nz - 1, nz)}
    north = {"gy": lax.rem(gy + 1, ny)}
    south = {"gy": lax.rem(gy + ny - 1, ny)}
    east = {"gx": lax.rem(gx + 1, nx)}
    west = {"gx": lax.rem(gx + nx - 1, nx)}
    mid_y = pl.ds(8, ys)
    mid_z = pl.ds(4, zs)
    halos = [
        send(0, xe.at[pl.ds(zs, 4), mid_y, :], xe.at[pl.ds(0, 4), mid_y, :], up),
        send(1, xe.at[pl.ds(4, 4), mid_y, :], xe.at[pl.ds(zs + 4, 4), mid_y, :], down),
        send(2, xe.at[mid_z, pl.ds(ys, 8), :], xe.at[mid_z, pl.ds(0, 8), :], north),
        send(3, xe.at[mid_z, pl.ds(8, 8), :], xe.at[mid_z, pl.ds(ys + 8, 8), :], south),
        send(4, xp, xl, east),
        send(5, xp, xr, west),
    ]
    for copy in halos:
        copy.wait()

    def correct(p, carry):
        e = jnp.where(part < 4, xl[p], xr[p]) - xp[p]
        high = jnp.where(part >= 4, e, 0.0)
        low = jnp.where(part < 4, e, 0.0)
        ahead = jnp.zeros((8, lanes), F32)
        behind = jnp.zeros((8, lanes), F32)
        for k, c in enumerate(COEF, start=1):
            ahead = ahead + c * pltpu.roll(high, lanes - k, 1)
            behind = behind + c * pltpu.roll(low, k, 1)
        corr[p] = jnp.where(part < 4, ahead, -behind)
        return carry

    lax.fori_loop(0, zs // 2, correct, 0)

    lower = first_ref[0].astype(F32)
    upper = beyond_ref[0].astype(F32)
    edge = (lane < 4) | (lane >= lanes - 4)
    half = jnp.where(iota((16, lanes), 0) < 8, 0.0, 1.0).astype(BF)
    one = jnp.ones((16, lanes), BF)
    zero = jnp.zeros((16, lanes), BF)

    def twice(v):
        return jnp.concatenate([v, v], axis=0).astype(BF)

    def planes(p, carry):
        total, most, least = carry
        for sub in range(2):
            z = 2 * p + sub
            left, right = [], []
            for t in range(tiles):
                row = 8 + 8 * t
                tile = xe[4 + z, pl.ds(row, 8), :]
                rz = jnp.zeros((8, lanes), F32)
                ry = jnp.zeros((8, lanes), F32)
                rx = jnp.where(edge, pltpu.roll(corr[p], (lanes - 8 * (8 * sub + t) - 4) % lanes, 1), 0.0)
                for k, c in enumerate(COEF, start=1):
                    rz = rz + c * (xe[4 + z + k, pl.ds(row, 8), :] - xe[4 + z - k, pl.ds(row, 8), :])
                    ry = ry + c * (xe[4 + z, pl.ds(row + k, 8), :] - xe[4 + z, pl.ds(row - k, 8), :])
                    rx = rx + c * (pltpu.roll(tile, lanes - k, 1) - pltpu.roll(tile, k, 1))
                m = jnp.sqrt(rz * rz + ry * ry + rx * rx + 1.0) - 1.0
                mag[z, pl.ds(8 * t, 8), :] = m
                position = jnp.clip(m * (BINS / RANGE), 0.5, BINS - 0.5) - 0.5
                low = jnp.minimum(jnp.floor(position), BINS - 2.0)
                frac = position - low
                weight = jnp.where((low >= lower) & (low < upper), 1.0 - frac, 0.0) + jnp.where(
                    (low + 1.0 >= lower) & (low + 1.0 < upper), frac, 0.0)
                wm = weight * m
                total = total + wm
                most = jnp.maximum(most, wm)
                least = jnp.minimum(least, m + RANGE * (1.0 - weight))
                coarse = jnp.floor((low + 0.5) * (1.0 / FINE))
                fine = low - FINE * coarse
                big = jnp.floor(frac * 256.0 + 0.5) * (1.0 / 256.0)
                c2 = twice(coarse) - half
                f2 = twice(fine) - half
                th, tl = twice(big), twice(frac - big)
                sh, sl = one - th, zero - tl
                left.append(jnp.concatenate(
                    [jnp.where(c2 == 2.0 * i, one, zero) for i in range(COARSE // 2)], axis=0))
                his, los = [], []
                for i in range(COLS // 2):
                    here, before = f2 == 2.0 * i, f2 == 2.0 * i - 1.0
                    his.append(jnp.where(here, sh, jnp.where(before, th, zero)))
                    los.append(jnp.where(here, sl, jnp.where(before, tl, zero)))
                right.append(jnp.concatenate(his + los, axis=0))
            acc[...] += lax.dot_general(
                jnp.concatenate(left, axis=1), jnp.concatenate(right, axis=1),
                (((1,), (1,)), ((), ())), preferred_element_type=F32)
        return total, most, least

    start = jnp.zeros((8, lanes), F32)
    total, most, least = lax.fori_loop(0, zs // 2, planes, (start, start - jnp.inf, start + jnp.inf))

    store = pltpu.make_async_copy(mag, mag_ref, out_sem)
    store.start()

    rows, cols = 8 * COARSE, 16 * COLS
    prod = jnp.where(iota((rows, cols), 0) % 8 == iota((rows, cols), 1) % 8, acc[...], 0.0)
    table = jnp.sum(prod.reshape(COARSE, 8, cols), axis=1)
    col = (iota((cols, BINS), 0) // 8) % COLS
    bin_ = iota((cols, BINS), 1)
    same = jnp.where(col == bin_ % FINE, 1.0, 0.0)
    over = jnp.where((col == FINE) & (bin_ % FINE == 0), 1.0, 0.0)
    crow = iota((COARSE, BINS), 0)
    cbin = iota((COARSE, BINS), 1) // FINE

    def spread(pick):
        return lax.dot_general(table, pick, (((1,), (0,)), ((), ())), precision=lax.Precision.HIGHEST,
                               preferred_element_type=F32)

    counts = jnp.sum(jnp.where(crow == cbin, spread(same), 0.0) + jnp.where(crow + 1 == cbin, spread(over), 0.0),
                     axis=0, keepdims=True)
    r4, l4 = iota((4, 128), 0), iota((4, 128), 1)
    mine = jnp.where(r4 == 0, counts[:, :128], jnp.where(r4 == 1, counts[:, 128:], 0.0))
    mine = jnp.where((r4 == 2) & (l4 == 0), jnp.sum(total), mine)
    mine = jnp.where((r4 == 2) & (l4 == 1), jnp.max(most), mine)
    mine = jnp.where((r4 == 2) & (l4 == 2), -jnp.min(least), mine)
    is_max = (r4 == 2) & (l4 >= 1)

    def exchange(value, buffer, place, peers, send_sem, recv_sem):
        own[...] = value
        buffer[place] = value
        copies = []
        for i, peer in enumerate(peers):
            copy = pltpu.make_async_remote_copy(
                src_ref=own, dst_ref=buffer.at[place], send_sem=send_sem.at[i], recv_sem=recv_sem.at[i],
                device_id=peer, device_id_type=MESH)
            copy.start()
            copies.append(copy)
        for copy in copies:
            copy.wait()
        added, top = buffer[0], buffer[0]
        for i in range(1, buffer.shape[0]):
            added = added + buffer[i]
            top = jnp.maximum(top, buffer[i])
        return jnp.where(is_max, top, added)

    mine = exchange(mine, plane, gx * nz + gz, plane_peers, plane_send, plane_recv)
    mine = exchange(mine, line, gy, line_peers, line_send, line_recv)

    bins = l4 + 128 * r4
    in_window = (r4 < 2) & (bins >= first_ref[0]) & (bins < beyond_ref[0])
    count = jnp.sum(jnp.where(in_window, mine, 0.0))

    def lane_of(i):
        return jnp.sum(jnp.where((r4 == 2) & (l4 == i), mine, 0.0))

    hist_ref[...] = (mine * (BINS / cells))[:2]
    lo, hi, s = -lane_of(2), lane_of(1), lane_of(0) / cells
    l1 = iota((1, 128), 1)
    stat_ref[...] = jnp.where(l1 == 0, lo, jnp.where(l1 == 1, hi, jnp.where(l1 == 2, s, count / cells)))
    store.wait()


def solution(mesh):
    nx, ny, nz = mesh.shape["gx"], mesh.shape["gy"], mesh.shape["gz"]

    def on_device(x, first, beyond):
        zs, ys, xs = x.shape
        cells = float(zs * ys * xs * nx * ny * nz)
        vmem = pl.BlockSpec(memory_space=pltpu.VMEM)
        smem = pl.BlockSpec(memory_space=pltpu.SMEM)
        hbm = pl.BlockSpec(memory_space=pl.ANY)
        dma = pltpu.SemaphoreType.DMA
        mag, hist, stat = pl.pallas_call(
            lambda *refs: kernel(nx, ny, nz, cells, *refs),
            name="field",
            out_shape=(
                jax.ShapeDtypeStruct(x.shape, F32),
                jax.ShapeDtypeStruct((2, 128), F32),
                jax.ShapeDtypeStruct((1, 128), F32),
            ),
            in_specs=[smem, smem, hbm],
            out_specs=(hbm, vmem, vmem),
            scratch_shapes=[
                pltpu.VMEM((zs + 8, ys + 16, xs), F32),
                pltpu.VMEM((zs // 2, 8, xs), F32),
                pltpu.VMEM((zs // 2, 8, xs), F32),
                pltpu.VMEM((zs // 2, 8, xs), F32),
                pltpu.VMEM((zs // 2, 8, xs), F32),
                pltpu.VMEM((zs, ys, xs), F32),
                pltpu.VMEM((8 * COARSE, 16 * COLS), F32),
                pltpu.VMEM((4, 128), F32),
                pltpu.VMEM((nx * nz, 4, 128), F32),
                pltpu.VMEM((ny, 4, 128), F32),
                dma, dma, dma((6,)), dma((6,)),
                dma((nx * nz - 1,)), dma((nx * nz - 1,)), dma((ny - 1,)), dma((ny - 1,)),
            ],
            compiler_params=pltpu.CompilerParams(collective_id=0, has_side_effects=True),
        )(first, beyond, x)
        return mag, hist.reshape(BINS), stat[0, :4]

    return jax.shard_map(
        on_device, mesh=mesh,
        in_specs=(P("gz", "gy", "gx"), P(), P()),
        out_specs=(P("gz", "gy", "gx"), P(), P()),
        check_vma=False,
    )
```

```python
import jax
import jax.numpy as jnp
from jax import lax
from jax.experimental import pallas as pl
from jax.experimental.pallas import tpu as pltpu
from jax.sharding import PartitionSpec as P

BINS = 256
RANGE = 12.0
COEF = (0.8, -0.2, 4.0 / 105.0, -1.0 / 280.0)
RATIO = tuple(c / COEF[0] for c in COEF)
FINE = 10
COARSE = 26
ROWS, COLS = 8 * COARSE, 24 * FINE
ROUND = 49152.0
MESH = pl.DeviceIdType.MESH
BF = jnp.bfloat16
F32 = jnp.float32


def iota(shape, dim):
    return lax.broadcasted_iota(jnp.int32, shape, dim)


def twice(v):
    return jnp.concatenate([v, v], axis=0).astype(BF)


def kernel(nx, ny, nz, cells, window, x_ref, mag, fin,
           xe, xph, xpl, xrh, xrl, yph, ypl, yrh, yrl, corh, corl, pick, acc, own, plane, line,
           in_sem, halo_send, halo_recv, plane_sem, line_sem, known):
    gx, gy, gz = lax.axis_index("gx"), lax.axis_index("gy"), lax.axis_index("gz")
    zs, ys, lanes = x_ref.shape
    tiles = ys // 8

    def away(axis, d):
        here, size = {"gx": (gx, nx), "gy": (gy, ny), "gz": (gz, nz)}[axis]
        return {axis: lax.rem(here + d % size, size)}

    def tell(sem, peers):
        for peer in peers:
            pl.semaphore_signal(sem, inc=1, device_id=peer, device_id_type=MESH)

    near = [away(axis, d) for axis in ("gx", "gy", "gz") for d in (1, -1)]
    barrier = pltpu.get_barrier_semaphore()
    load = pltpu.make_async_copy(x_ref, xe.at[pl.ds(4, zs), pl.ds(8, ys), :], in_sem)
    load.start()
    tell(barrier, near)

    lane = iota((8, lanes), 1)
    sub = iota((8, lanes), 0)
    group, part = lane // 4, lane % 4
    acc[...] = jnp.zeros_like(acc)
    kind, digit = iota((COLS, BINS), 0) // (8 * FINE), (iota((COLS, BINS), 0) // 8) % FINE
    bin_ = iota((COLS, BINS), 1)
    picked = jnp.where(digit == bin_ % FINE, jnp.where(kind == 0, 1.0, -1.0), 0.0)
    moved = jnp.where((digit == (bin_ + FINE - 1) % FINE) & (kind > 0), 1.0, 0.0)
    pick[:, :BINS] = picked.astype(BF)
    pick[:, BINS:] = moved.astype(BF)

    load.wait()

    def pack_y(i, carry):
        z = 4 + 2 * i
        yph[i] = jnp.where(sub < 4, xe[z, pl.ds(ys + 4, 8), :], xe[z + 1, pl.ds(ys, 8), :])
        ypl[i] = jnp.where(sub < 4, xe[z, pl.ds(8, 8), :], xe[z + 1, pl.ds(4, 8), :])
        return carry

    def pack_x(p, carry):
        high = jnp.zeros((8, lanes), F32)
        low = jnp.zeros((8, lanes), F32)
        for g in range(32):
            tile = xe[4 + 4 * p + g // 8, pl.ds(8 + 8 * (g % 8), 8), :]
            high = jnp.where(group == g, pltpu.roll(tile, (4 + 4 * g) % lanes, 1), high)
            low = jnp.where(group == g, pltpu.roll(tile, 4 * g, 1) if g else tile, low)
        xph[p] = high
        xpl[p] = low
        return carry

    lax.fori_loop(0, zs // 2, pack_y, 0)
    lax.fori_loop(0, zs // 4, pack_x, 0)
    pl.semaphore_wait(barrier, len(near))

    def send(i, src, dst, peer):
        copy = pltpu.make_async_remote_copy(
            src_ref=src, dst_ref=dst, send_sem=halo_send.at[i], recv_sem=halo_recv.at[i],
            device_id=peer, device_id_type=MESH)
        copy.start()
        return copy

    mid_y = pl.ds(8, ys)
    sides = [
        send(0, xph, xrh, away("gx", 1)),
        send(1, xpl, xrl, away("gx", -1)),
        send(2, yph, yrh, away("gy", 1)),
        send(3, ypl, yrl, away("gy", -1)),
    ]
    depths = [
        send(4, xe.at[pl.ds(zs, 4), mid_y, :], xe.at[pl.ds(0, 4), mid_y, :], away("gz", 1)),
        send(5, xe.at[pl.ds(4, 4), mid_y, :], xe.at[pl.ds(zs + 4, 4), mid_y, :], away("gz", -1)),
    ]
    tell(known.at[0], near)
    for copy in sides:
        copy.wait()

    def unpack_y(i, carry):
        z = 4 + 2 * i
        below, above = yrh[i], yrl[i]
        xe[z, pl.ds(4, 4), :] = below[:4]
        xe[z + 1, pl.ds(4, 4), :] = below[4:]
        xe[z, pl.ds(ys + 8, 4), :] = above[:4]
        xe[z + 1, pl.ds(ys + 8, 4), :] = above[4:]
        return carry

    def correct(p, carry):
        left = xrh[p] - xph[p]
        right = xrl[p] - xpl[p]
        ahead = RATIO[3] * right
        behind = RATIO[3] * left
        for k in range(1, 4):
            ahead = ahead + jnp.where(part >= 4 - k, RATIO[k - 1] * pltpu.roll(right, 4 - k, 1), 0.0)
            behind = behind + jnp.where(part < k, RATIO[k - 1] * pltpu.roll(left, lanes - 4 + k, 1), 0.0)
        corh[p] = ahead
        corl[p] = -behind
        return carry

    lax.fori_loop(0, zs // 2, unpack_y, 0)
    lax.fori_loop(0, zs // 4, correct, 0)
    pl.semaphore_wait(known.at[0], len(near))
    tell(known.at[1], [away(axis, d) for axis in ("gy", "gz") for d in (2, -2)])

    first, upper = window[:1], window[1:]
    lower = first - 1.0
    half = jnp.where(iota((16, lanes), 0) < 8, 0.0, 1.0).astype(BF)
    one = jnp.ones((16, lanes), BF)
    zero = jnp.zeros((16, lanes), BF)

    def planes(turn, carry):
        total, most, least = carry
        p = lax.rem(turn + 1, zs // 4)
        product = None
        for sub_z in range(4):
            z = 4 * p + sub_z
            left, right = [], []
            for t in range(tiles):
                row = 8 + 8 * t
                g = 8 * sub_z + t
                tile = xe[4 + z, pl.ds(row, 8), :]
                rx = jnp.where(lane >= lanes - 4, pltpu.roll(corh[p], (lanes - 4 - 4 * g) % lanes, 1),
                               jnp.where(lane < 4, pltpu.roll(corl[p], (lanes - 4 * g) % lanes, 1), 0.0))
                ry, rz = None, None
                for k, c in enumerate(RATIO, start=1):
                    dz = xe[4 + z + k, pl.ds(row, 8), :] - xe[4 + z - k, pl.ds(row, 8), :]
                    dy = xe[4 + z, pl.ds(row + k, 8), :] - xe[4 + z, pl.ds(row - k, 8), :]
                    dx = pltpu.roll(tile, lanes - k, 1) - pltpu.roll(tile, k, 1)
                    rz = dz if rz is None else rz + c * dz
                    ry = dy if ry is None else ry + c * dy
                    rx = rx + (dx if k == 1 else c * dx)
                square = (rz * rz + ry * ry + rx * rx) * (COEF[0] * COEF[0]) + 1.0
                m = square * lax.rsqrt(square) - 1.0
                mag[z, pl.ds(8 * t, 8), :] = m
                q = jnp.minimum(jnp.maximum(m * (BINS / RANGE) - 0.5, 0.0), BINS - 1.0)
                low = jnp.minimum(jnp.floor(q), BINS - 2.0)
                frac = q - low
                weight = jnp.maximum(jnp.minimum(jnp.minimum(q - lower, 1.0), upper - q), 0.0)
                wm = weight * m
                total = total + wm
                most = jnp.maximum(most, wm)
                least = jnp.minimum(least, m + RANGE * (1.0 - weight))
                coarse = jnp.floor((low + 0.5) * (1.0 / FINE))
                fine = low - FINE * coarse
                big = (frac + ROUND) - ROUND
                c2 = twice(coarse) - half
                f2 = twice(fine) - half
                th, tl = twice(big), twice(frac - big)
                left.append(jnp.concatenate(
                    [jnp.where(c2 == 2.0 * i, one, zero) for i in range(COARSE // 2)], axis=0))
                here = [f2 == 2.0 * i for i in range(FINE // 2)]
                right.append(jnp.concatenate(
                    [jnp.where(h, v, zero) for v in (one, th, tl) for h in here], axis=0))
            dot = lax.dot_general(
                jnp.concatenate(left, axis=1), jnp.concatenate(right, axis=1),
                (((1,), (1,)), ((), ())), preferred_element_type=F32)
            product = dot if product is None else product + dot
        acc[...] += product
        return total, most, least

    start = jnp.zeros((8, lanes), F32)
    state = (start, start - jnp.inf, start + jnp.inf)
    inner = zs // 4 - 2
    state = lax.fori_loop(0, inner, planes, state)
    for copy in depths:
        copy.wait()
    pl.semaphore_wait(known.at[1], 4)
    tell(known.at[2], [away("gy", 4), away("gy", -4)] + [away("gx", d) for d in range(1, nx)])
    total, most, least = lax.fori_loop(inner, zs // 4, planes, state)

    prod = jnp.where(iota((ROWS, COLS), 0) % 8 == iota((ROWS, COLS), 1) % 8, acc[...], 0.0)
    table = jnp.sum(prod.reshape(COARSE, 8, COLS), axis=1)
    one_part = table.astype(BF)
    rest = table - one_part.astype(F32)
    two_part = rest.astype(BF)
    three_part = (rest - two_part.astype(F32)).astype(BF)
    crow = iota((COARSE, BINS), 0)
    cbin = iota((COARSE, BINS), 1)

    def spread(v):
        return lax.dot_general(v, pick[...], (((1,), (0,)), ((), ())), preferred_element_type=F32)

    wide = spread(one_part) + spread(two_part) + spread(three_part)
    counts = jnp.sum(
        jnp.where(crow == cbin // FINE, wide[:, :BINS], 0.0)
        + jnp.where(crow + 1 == (cbin + FINE - 1) // FINE, wide[:, BINS:], 0.0),
        axis=0, keepdims=True)
    r4, l4 = iota((4, 128), 0), iota((4, 128), 1)
    mine = jnp.where(r4 == 0, counts[:, :128], jnp.where(r4 == 1, counts[:, 128:], 0.0))
    mine = jnp.where((r4 == 2) & (l4 == 0), jnp.sum(total), mine)
    mine = jnp.where((r4 == 2) & (l4 == 1), jnp.max(most), mine)
    mine = jnp.where((r4 == 2) & (l4 == 2), -jnp.min(least), mine)
    is_max = (r4 == 2) & (l4 >= 1)

    def exchange(value, buffer, place, peers, sems):
        own[...] = value
        buffer[place] = value
        for peer in peers:
            pltpu.make_async_remote_copy(
                src_ref=own, dst_ref=buffer.at[place], send_sem=sems.at[0], recv_sem=sems.at[1],
                device_id=peer, device_id_type=MESH).start()
        every = buffer.at[pl.ds(0, len(peers))]
        pltpu.make_async_copy(every, every, sems.at[1]).wait()
        pltpu.make_async_copy(every, every, sems.at[0]).wait()
        added, top = buffer[0], buffer[0]
        for i in range(1, buffer.shape[0]):
            added = added + buffer[i]
            top = jnp.maximum(top, buffer[i])
        return jnp.where(is_max, top, added)

    pl.semaphore_wait(known.at[2], nx + 1)
    mine = exchange(mine, plane, gx * nz + gz,
                    [away("gx", dx) | away("gz", dz) for dx in range(nx) for dz in range(nz) if dx or dz],
                    plane_sem)
    mine = exchange(mine, line, gy, [away("gy", d) for d in range(1, ny)], line_sem)

    bins = (l4 + 128 * r4).astype(F32)
    count = jnp.sum(jnp.where((r4 < 2) & (bins >= first) & (bins < upper), mine, 0.0))

    def lane_of(i):
        return jnp.sum(jnp.where((r4 == 2) & (l4 == i), mine, 0.0))

    stats = jnp.where(l4 == 0, -lane_of(2), jnp.where(
        l4 == 1, lane_of(1), jnp.where(l4 == 2, lane_of(0) / cells, count / cells)))
    fin[...] = jnp.where(r4 < 2, mine * (BINS / cells), stats)


def finish(mag, fin, mag_ref, hist_ref, stat_ref, sem):
    store = pltpu.make_async_copy(mag, mag_ref, sem)
    store.start()
    hist_ref[...] = fin[:2]
    stat_ref[...] = fin[2:3, :4]
    store.wait()


def solution(mesh):
    nx, ny, nz = mesh.shape["gx"], mesh.shape["gy"], mesh.shape["gz"]

    def on_device(x, first, beyond):
        zs, ys, xs = x.shape
        cells = float(zs * ys * xs * nx * ny * nz)
        vmem = pl.BlockSpec(memory_space=pltpu.VMEM)
        hbm = pl.BlockSpec(memory_space=pltpu.HBM)
        dma = pltpu.SemaphoreType.DMA
        x_pack = pltpu.VMEM((zs // 4, 8, xs), F32)
        y_pack = pltpu.VMEM((zs // 2, 8, xs), F32)
        window = jnp.concatenate([jnp.broadcast_to(v.astype(F32), (1, xs)) for v in (first, beyond)])
        window = pltpu.with_memory_space_constraint(window, pltpu.VMEM)
        mag, fin = pl.pallas_call(
            lambda *refs: kernel(nx, ny, nz, cells, *refs),
            name="field",
            out_shape=(pltpu.VMEM(x.shape, F32), pltpu.VMEM((4, 128), F32)),
            in_specs=[vmem, hbm],
            out_specs=(vmem, vmem),
            scratch_shapes=[
                pltpu.VMEM((zs + 8, ys + 16, xs), F32),
                x_pack, x_pack, x_pack, x_pack,
                y_pack, y_pack, y_pack, y_pack,
                x_pack, x_pack,
                pltpu.VMEM((COLS, 2 * BINS), BF),
                pltpu.VMEM((ROWS, COLS), F32),
                pltpu.VMEM((4, 128), F32),
                pltpu.VMEM((nx * nz, 4, 128), F32),
                pltpu.VMEM((ny, 4, 128), F32),
                dma, dma((6,)), dma((6,)), dma((2,)), dma((2,)),
                pltpu.SemaphoreType.REGULAR((3,)),
            ],
            compiler_params=pltpu.CompilerParams(collective_id=0, has_side_effects=True),
        )(window, x)
        mag, fin = (pltpu.with_memory_space_constraint(v, pltpu.VMEM) for v in (mag, fin))
        mag, hist, stat = pl.pallas_call(
            finish,
            name="finish",
            out_shape=(
                jax.ShapeDtypeStruct(x.shape, F32),
                jax.ShapeDtypeStruct((2, 128), F32),
                jax.ShapeDtypeStruct((1, 4), F32),
            ),
            in_specs=[vmem, vmem],
            out_specs=(hbm, vmem, vmem),
            scratch_shapes=[dma],
        )(mag, fin)
        return mag, hist.reshape(BINS), stat.reshape(4)

    return jax.shard_map(
        on_device, mesh=mesh,
        in_specs=(P("gz", "gy", "gx"), P(), P()),
        out_specs=(P("gz", "gy", "gx"), P(), P()),
        check_vma=False,
    )
```

```python
import jax
import jax.numpy as jnp
from jax import lax
from jax.experimental import pallas as pl
from jax.experimental.pallas import tpu as pltpu
from jax.sharding import PartitionSpec as P

BINS = 256
RANGE = 12.0
COEF = (0.8, -0.2, 4.0 / 105.0, -1.0 / 280.0)
RATIO = tuple(c / COEF[0] for c in COEF)
FINE = 10
COARSE = 26
ROWS, COLS = 8 * COARSE, 24 * FINE
ROUND = 49152.0
MESH = pl.DeviceIdType.MESH
BF = jnp.bfloat16
F32 = jnp.float32


def iota(shape, dim):
    return lax.broadcasted_iota(jnp.int32, shape, dim)


def twice(v):
    return jnp.concatenate([v, v], axis=0).astype(BF)


def kernel(nx, ny, nz, cells, window, x_ref, mag, hist, stat,
           xe, xp, xl, xr, yph, ypl, yrh, yrl, flat, bend, rim, pick, acc, own, plane, line,
           in_sem, halo_send, halo_recv, plane_sem, line_sem, known):
    gx, gy, gz = lax.axis_index("gx"), lax.axis_index("gy"), lax.axis_index("gz")
    zs, ys, lanes = x_ref.shape
    tiles = ys // 8

    def away(axis, d):
        here, size = {"gx": (gx, nx), "gy": (gy, ny), "gz": (gz, nz)}[axis]
        return {axis: lax.rem(here + d % size, size)}

    def tell(sem, peers):
        for peer in peers:
            pl.semaphore_signal(sem, inc=1, device_id=peer, device_id_type=MESH)

    near = [away(axis, d) for axis in ("gx", "gy", "gz") for d in (1, -1)]
    barrier = pltpu.get_barrier_semaphore()
    load = pltpu.make_async_copy(x_ref, xe.at[pl.ds(4, zs), pl.ds(8, ys), :], in_sem)
    load.start()
    tell(barrier, near)

    lane = iota((8, lanes), 1)
    sub = iota((8, lanes), 0)
    group, part = lane // 8, lane % 8
    acc[...] = jnp.zeros_like(acc)
    kind, digit = iota((COLS, BINS), 0) // (8 * FINE), (iota((COLS, BINS), 0) // 8) % FINE
    bin_ = iota((COLS, BINS), 1)
    picked = jnp.where(digit == bin_ % FINE, jnp.where(kind == 0, 1.0, -1.0), 0.0)
    moved = jnp.where((digit == (bin_ + FINE - 1) % FINE) & (kind > 0), 1.0, 0.0)
    pick[:, :BINS] = picked.astype(BF)
    pick[:, BINS:] = moved.astype(BF)

    load.wait()

    def pack_y(i, carry):
        z = 4 + 2 * i
        yph[i] = jnp.where(sub < 4, xe[z, pl.ds(ys + 4, 8), :], xe[z + 1, pl.ds(ys, 8), :])
        ypl[i] = jnp.where(sub < 4, xe[z, pl.ds(8, 8), :], xe[z + 1, pl.ds(4, 8), :])
        return carry

    def pack_x(p, carry):
        packed = jnp.zeros((8, lanes), F32)
        for g in range(16):
            tile = xe[4 + 2 * p + g // 8, pl.ds(8 + 8 * (g % 8), 8), :]
            packed = jnp.where(group == g, pltpu.roll(tile, (4 + 8 * g) % lanes, 1), packed)
        xp[p] = packed
        return carry

    lax.fori_loop(0, zs // 2, pack_y, 0)
    lax.fori_loop(0, zs // 2, pack_x, 0)
    pl.semaphore_wait(barrier, len(near))

    def send(i, src, dst, peer):
        copy = pltpu.make_async_remote_copy(
            src_ref=src, dst_ref=dst, send_sem=halo_send.at[i], recv_sem=halo_recv.at[i],
            device_id=peer, device_id_type=MESH)
        copy.start()
        return copy

    mid_y = pl.ds(8, ys)
    rows_y = [
        send(2, yph, yrh, away("gy", 1)),
        send(3, ypl, yrl, away("gy", -1)),
    ]
    depths = [
        send(4, xe.at[pl.ds(zs, 4), mid_y, :], xe.at[pl.ds(0, 4), mid_y, :], away("gz", 1)),
        send(5, xe.at[pl.ds(4, 4), mid_y, :], xe.at[pl.ds(zs + 4, 4), mid_y, :], away("gz", -1)),
    ]
    rows_x = [
        send(0, xp, xl, away("gx", 1)),
        send(1, xp, xr, away("gx", -1)),
    ]
    tell(known.at[0], near)

    def unpack_y(i, carry):
        z = 4 + 2 * i
        below, above = yrh[i], yrl[i]
        xe[z, pl.ds(4, 4), :] = below[:4]
        xe[z + 1, pl.ds(4, 4), :] = below[4:]
        xe[z, pl.ds(ys + 8, 4), :] = above[:4]
        xe[z + 1, pl.ds(ys + 8, 4), :] = above[4:]
        return carry

    first, upper = window[:1], window[1:]
    lower = first - 1.0
    half = jnp.where(iota((16, lanes), 0) < 8, 0.0, 1.0).astype(BF)
    one = jnp.ones((16, lanes), BF)
    zero = jnp.zeros((16, lanes), BF)

    edge = (lane < 4) | (lane >= lanes - 4)

    def slope(z, t):
        row = 8 + 8 * t
        tile = xe[4 + z, pl.ds(row, 8), :]
        rx, ry, rz = None, None, None
        for k, c in enumerate(RATIO, start=1):
            dz = xe[4 + z + k, pl.ds(row, 8), :] - xe[4 + z - k, pl.ds(row, 8), :]
            dy = xe[4 + z, pl.ds(row + k, 8), :] - xe[4 + z, pl.ds(row - k, 8), :]
            dx = pltpu.roll(tile, lanes - k, 1) - pltpu.roll(tile, k, 1)
            rz = dz if rz is None else rz + c * dz
            ry = dy if ry is None else ry + c * dy
            rx = dx if rx is None else rx + c * dx
        return rz * rz + ry * ry, rx

    def cell(square, state, masked):
        total, most, least = state
        square = square * (COEF[0] * COEF[0]) + 1.0
        m = square * lax.rsqrt(square) - 1.0
        q = jnp.minimum(jnp.maximum(m * (BINS / RANGE) - 0.5, 0.0), BINS - 1.0)
        low = jnp.floor(q)
        frac = q - low
        weight = jnp.maximum(jnp.minimum(jnp.minimum(q - lower, 1.0), upper - q), 0.0)
        if masked:
            weight = jnp.where(edge, 0.0, weight)
        wm = weight * m
        under = m - RANGE * weight
        if masked:
            under = jnp.where(edge, jnp.inf, under)
        state = total + wm, jnp.maximum(most, wm), jnp.minimum(least, under)
        coarse = jnp.floor((low + 0.5) * (1.0 / FINE))
        fine = low - FINE * coarse
        if masked:
            coarse = jnp.where(edge, -64.0, coarse)
        th = twice(frac)
        tl = twice(frac - th[:8].astype(F32))
        c2 = twice(coarse) - half
        f2 = twice(fine) - half
        here = [f2 == 2.0 * i for i in range(FINE // 2)]
        left = jnp.concatenate([jnp.where(c2 == 2.0 * i, one, zero) for i in range(COARSE // 2)], axis=0)
        right = jnp.concatenate([jnp.where(h, v, zero) for v in (one, th, tl) for h in here], axis=0)
        return m, state, left, right

    def gather(pairs):
        product = None
        for at in range(0, len(pairs), 8):
            left, right = zip(*pairs[at:at + 8])
            dot = lax.dot_general(
                jnp.concatenate(left, axis=1), jnp.concatenate(right, axis=1),
                (((1,), (1,)), ((), ())), preferred_element_type=F32)
            product = dot if product is None else product + dot
        acc[...] += product

    def body(places, state, chosen, fresh):
        pairs = []
        for z, odd in places:
            if not odd:
                flats = jnp.zeros((8, lanes), F32) if fresh else flat[z // 2]
                bends = jnp.zeros((8, lanes), F32) if fresh else bend[z // 2]
            for t in chosen:
                g = 8 * odd + t
                square, rx = slope(z, t)
                flats = jnp.where(group == g, pltpu.roll(square, (4 + 8 * g) % lanes, 1), flats)
                bends = jnp.where(group == g, pltpu.roll(rx, (4 + 8 * g) % lanes, 1), bends)
                m, state, left, right = cell(square + rx * rx, state, True)
                mag[z, pl.ds(8 * t, 8), :] = m
                pairs.append((left, right))
            if odd:
                flat[z // 2] = flats
                bend[z // 2] = bends
        return pairs, state

    inner = range(1, tiles - 1)
    outer = (0, tiles - 1)

    def middle(turn, state):
        @pl.when(turn == 1)
        def _():
            pl.semaphore_wait(known.at[0], len(near))
            tell(known.at[1], [away(axis, d) for axis in ("gy", "gz") for d in (2, -2)])

        pairs, state = body([(4 + 8 * turn + i, i % 2) for i in range(8)], state, inner, True)
        gather(pairs)
        return state

    start = jnp.zeros((8, lanes), F32)
    state = (start, start - jnp.inf, start + jnp.inf)
    thirds = (zs - 8) // 8
    state = lax.fori_loop(0, thirds, middle, state)
    pl.semaphore_wait(known.at[1], 4)
    tell(known.at[2], [away("gy", 4), away("gy", -4)] + [away("gx", d) for d in range(1, nx)])
    for copy in rows_y + depths + rows_x:
        copy.wait()
    lax.fori_loop(0, zs // 2, unpack_y, 0)

    pairs, state = body([(z, z % 2) for z in range(4, zs - 4)], state, outer, False)
    more, state = body([(z, z % 2) for z in range(zs) if z < 4 or z >= zs - 4], state, range(tiles), True)
    pairs = pairs + more
    for p in range(zs // 2):
        e = jnp.where(part < 4, xl[p], xr[p]) - xp[p]
        high = jnp.where(part >= 4, e, 0.0)
        low = jnp.where(part < 4, e, 0.0)
        ahead, behind = 0.0, 0.0
        for k, c in enumerate(RATIO, start=1):
            ahead = ahead + c * pltpu.roll(high, lanes - k, 1)
            behind = behind + c * pltpu.roll(low, k, 1)
        rx = bend[p] + jnp.where(part < 4, ahead, -behind)
        m, state, left, right = cell(flat[p] + rx * rx, state, False)
        rim[p] = m
        pairs.append((left, right))
    gather(pairs)
    total, most, least = state

    def mend(p, carry):
        for g in range(16):
            place = (2 * p + g // 8, pl.ds(8 * (g % 8), 8))
            mag[place] = jnp.where(edge, pltpu.roll(rim[p], (lanes - 4 - 8 * g) % lanes, 1), mag[place])
        return carry

    prod = jnp.where(iota((ROWS, COLS), 0) % 8 == iota((ROWS, COLS), 1) % 8, acc[...], 0.0)
    table = jnp.sum(prod.reshape(COARSE, 8, COLS), axis=1)
    one_part = table.astype(BF)
    rest = table - one_part.astype(F32)
    two_part = rest.astype(BF)
    three_part = (rest - two_part.astype(F32)).astype(BF)
    crow = iota((COARSE, BINS), 0)
    cbin = iota((COARSE, BINS), 1)

    def spread(v):
        return lax.dot_general(v, pick[...], (((1,), (0,)), ((), ())), preferred_element_type=F32)

    wide = spread(one_part) + spread(two_part) + spread(three_part)
    counts = jnp.sum(
        jnp.where(crow == cbin // FINE, wide[:, :BINS], 0.0)
        + jnp.where(crow + 1 == (cbin + FINE - 1) // FINE, wide[:, BINS:], 0.0),
        axis=0, keepdims=True)
    r4, l4 = iota((3, 128), 0), iota((3, 128), 1)
    mine = jnp.where(r4 == 0, counts[:, :128], jnp.where(r4 == 1, counts[:, 128:], 0.0))
    mine = jnp.where((r4 == 2) & (l4 == 0), jnp.sum(total), mine)
    mine = jnp.where((r4 == 2) & (l4 == 1), jnp.max(most), mine)
    mine = jnp.where((r4 == 2) & (l4 == 2), -RANGE - jnp.min(least), mine)
    is_max = (r4 == 2) & (l4 >= 1)

    def exchange(value, buffer, place, peers, sems, work=None):
        own[...] = value
        buffer[place] = value
        for peer in peers:
            pltpu.make_async_remote_copy(
                src_ref=own, dst_ref=buffer.at[place], send_sem=sems.at[0], recv_sem=sems.at[1],
                device_id=peer, device_id_type=MESH).start()
        if work is not None:
            work()
        every = buffer.at[pl.ds(0, len(peers))]
        pltpu.make_async_copy(every, every, sems.at[1]).wait()
        pltpu.make_async_copy(every, every, sems.at[0]).wait()
        added, top = buffer[0], buffer[0]
        for i in range(1, buffer.shape[0]):
            added = added + buffer[i]
            top = jnp.maximum(top, buffer[i])
        return jnp.where(is_max, top, added)

    pl.semaphore_wait(known.at[2], nx + 1)
    mine = exchange(mine, plane, gx * nz + gz,
                    [away("gx", dx) | away("gz", dz) for dx in (2, 1, 3, 0) for dz in (2, 6, 5, 3, 4, 1, 7, 0) if dx or dz],
                    plane_sem, lambda: lax.fori_loop(0, zs // 2, mend, 0))
    mine = exchange(mine, line, gy, [away("gy", d) for d in (8, 7, 9, 6, 10, 5, 11, 4, 12, 3, 13, 2, 14, 1, 15)], line_sem)

    bins = (l4 + 128 * r4).astype(F32)
    count = jnp.sum(jnp.where((r4 < 2) & (bins >= first) & (bins < upper), mine, 0.0))

    def lane_of(i):
        return jnp.sum(jnp.where((r4 == 2) & (l4 == i), mine, 0.0))

    l1 = iota((1, 4), 1)
    hist[...] = mine[:2] * (BINS / cells)
    stat[...] = jnp.where(l1 == 0, -lane_of(2), jnp.where(
        l1 == 1, lane_of(1), jnp.where(l1 == 2, lane_of(0) / cells, count / cells)))


def finish(mag, hist, stat, mag_ref, hist_ref, stat_ref, sems):
    copies = [
        pltpu.make_async_copy(source, target, sems.at[i])
        for i, (source, target) in enumerate(((mag, mag_ref), (hist, hist_ref), (stat, stat_ref)))
    ]
    for copy in copies:
        copy.start()
    for copy in copies:
        copy.wait()


def solution(mesh):
    nx, ny, nz = mesh.shape["gx"], mesh.shape["gy"], mesh.shape["gz"]

    def on_device(x, first, beyond):
        zs, ys, xs = x.shape
        cells = float(zs * ys * xs * nx * ny * nz)
        vmem = pl.BlockSpec(memory_space=pltpu.VMEM)
        hbm = pl.BlockSpec(memory_space=pltpu.HBM)
        dma = pltpu.SemaphoreType.DMA
        window = jnp.concatenate([jnp.broadcast_to(v.astype(F32), (1, xs)) for v in (first, beyond)])
        window = pltpu.with_memory_space_constraint(window, pltpu.VMEM)
        packed = pltpu.VMEM((zs // 2, 8, xs), F32)
        parts = pl.pallas_call(
            lambda *refs: kernel(nx, ny, nz, cells, *refs),
            name="field",
            out_shape=(pltpu.VMEM(x.shape, F32), pltpu.VMEM((2, 128), F32), pltpu.VMEM((1, 4), F32)),
            in_specs=[vmem, hbm],
            out_specs=(vmem, vmem, vmem),
            scratch_shapes=[
                pltpu.VMEM((zs + 8, ys + 16, xs), F32),
                packed, packed, packed,
                packed, packed, packed, packed,
                packed, packed, packed,
                pltpu.VMEM((COLS, 2 * BINS), BF),
                pltpu.VMEM((ROWS, COLS), F32),
                pltpu.VMEM((3, 128), F32),
                pltpu.VMEM((nx * nz, 3, 128), F32),
                pltpu.VMEM((ny, 3, 128), F32),
                dma, dma((6,)), dma((6,)), dma((2,)), dma((2,)),
                pltpu.SemaphoreType.REGULAR((3,)),
            ],
            compiler_params=pltpu.CompilerParams(collective_id=0, has_side_effects=True),
        )(window, x)
        parts = [pltpu.with_memory_space_constraint(v, pltpu.VMEM) for v in parts]
        mag, hist, stat = pl.pallas_call(
            finish,
            name="finish",
            out_shape=tuple(jax.ShapeDtypeStruct(v.shape, F32) for v in parts),
            in_specs=[vmem, vmem, vmem],
            out_specs=(hbm, hbm, hbm),
            scratch_shapes=[dma((3,))],
        )(*parts)
        return mag, hist.reshape(BINS), stat.reshape(4)

    return jax.shard_map(
        on_device, mesh=mesh,
        in_specs=(P("gz", "gy", "gx"), P(), P()),
        out_specs=(P("gz", "gy", "gx"), P(), P()),
        check_vma=False,
    )
```

```python
import jax
import jax.numpy as jnp
from jax import lax
from jax.experimental import pallas as pl
from jax.experimental.pallas import tpu as pltpu
from jax.sharding import PartitionSpec as P

BINS = 256
RANGE = 12.0
COEF = (0.8, -0.2, 4.0 / 105.0, -1.0 / 280.0)
RATIO = tuple(c / COEF[0] for c in COEF)
FINE = 10
COARSE = 26
ROWS, COLS = 8 * COARSE, 24 * FINE
ROUND = 49152.0
MESH = pl.DeviceIdType.MESH
BF = jnp.bfloat16
F32 = jnp.float32


def iota(shape, dim):
    return lax.broadcasted_iota(jnp.int32, shape, dim)


def twice(v):
    return jnp.concatenate([v, v], axis=0).astype(BF)


def kernel(nx, ny, nz, cells, window, x_ref, mag, hist, stat,
           xe, xp, xh, xw, xl, xr, yph, ypl, yrh, yrl, flat, bend, rim, pick, acc, own, plane, line,
           in_sem, halo_send, halo_recv, plane_sem, line_sem, known):
    gx, gy, gz = lax.axis_index("gx"), lax.axis_index("gy"), lax.axis_index("gz")
    zs, ys, lanes = x_ref.shape
    tiles = ys // 8

    def away(axis, d):
        here, size = {"gx": (gx, nx), "gy": (gy, ny), "gz": (gz, nz)}[axis]
        return {axis: lax.rem(here + d % size, size)}

    def tell(sem, peers):
        for peer in peers:
            pl.semaphore_signal(sem, inc=1, device_id=peer, device_id_type=MESH)

    near = [away(axis, d) for axis in ("gx", "gy", "gz") for d in (1, -1)]
    barrier = pltpu.get_barrier_semaphore()
    load = pltpu.make_async_copy(x_ref, xe.at[pl.ds(4, zs), pl.ds(8, ys), :], in_sem)
    for z in range(0, zs, 4):
        pltpu.make_async_copy(
            x_ref.at[pl.ds(z, 4)], xe.at[pl.ds(4 + z, 4), pl.ds(8, ys), :], in_sem).start()
    tell(barrier, near)

    lane = iota((8, lanes), 1)
    sub = iota((8, lanes), 0)
    group, part = lane // 8, lane % 8
    acc[...] = jnp.zeros_like(acc)
    kind, digit = iota((COLS, BINS), 0) // (8 * FINE), (iota((COLS, BINS), 0) // 8) % FINE
    bin_ = iota((COLS, BINS), 1)
    picked = jnp.where(digit == bin_ % FINE, jnp.where(kind == 0, 1.0, -1.0), 0.0)
    moved = jnp.where((digit == (bin_ + FINE - 1) % FINE) & (kind > 0), 1.0, 0.0)
    pick[:, :BINS] = picked.astype(BF)
    pick[:, BINS:] = moved.astype(BF)

    load.wait()

    def pack_y(i, carry):
        z = 4 + 2 * i
        yph[i] = jnp.where(sub < 4, xe[z, pl.ds(ys + 4, 8), :], xe[z + 1, pl.ds(ys, 8), :])
        ypl[i] = jnp.where(sub < 4, xe[z, pl.ds(8, 8), :], xe[z + 1, pl.ds(4, 8), :])
        return carry

    def pack_x(turn, carry):
        for i in range(4):
            p = 4 * turn + i
            packed = jnp.zeros((8, lanes), F32)
            for g in range(16):
                tile = xe[4 + 2 * p + g // 8, pl.ds(8 + 8 * (g % 8), 8), :]
                packed = jnp.where(group == g, pltpu.roll(tile, (4 + 8 * g) % lanes, 1), packed)
            xp[p] = packed
        return carry

    lax.fori_loop(0, zs // 2, pack_y, 0)
    pl.semaphore_wait(barrier, len(near))

    def send(i, src, dst, peer):
        copy = pltpu.make_async_remote_copy(
            src_ref=src, dst_ref=dst, send_sem=halo_send.at[i], recv_sem=halo_recv.at[i],
            device_id=peer, device_id_type=MESH)
        copy.start()
        return copy

    mid_y = pl.ds(8, ys)
    rows_y = [
        send(2, yph, yrh, away("gy", 1)),
        send(3, ypl, yrl, away("gy", -1)),
    ]
    depths = [
        send(4, xe.at[pl.ds(zs, 4), mid_y, :], xe.at[pl.ds(0, 4), mid_y, :], away("gz", 1)),
        send(5, xe.at[pl.ds(4, 4), mid_y, :], xe.at[pl.ds(zs + 4, 4), mid_y, :], away("gz", -1)),
    ]
    tell(known.at[0], near)
    lax.fori_loop(0, zs // 8, pack_x, 0)
    quarter = zs // 4
    for p in range(quarter):
        near_p, far_p = xp[p], xp[p + quarter]
        xh[p] = jnp.where(part < 4, near_p, pltpu.roll(far_p, 4, 1))
        xw[p] = jnp.where(part >= 4, near_p, pltpu.roll(far_p, lanes - 4, 1))
    rows_x = [
        send(0, xh, xl, away("gx", 1)),
        send(1, xw, xr, away("gx", -1)),
    ]

    def unpack_y(i, carry):
        z = 4 + 2 * i
        below, above = yrh[i], yrl[i]
        xe[z, pl.ds(4, 4), :] = below[:4]
        xe[z + 1, pl.ds(4, 4), :] = below[4:]
        xe[z, pl.ds(ys + 8, 4), :] = above[:4]
        xe[z + 1, pl.ds(ys + 8, 4), :] = above[4:]
        return carry

    lower, upper = window[:1] - 1.0, window[1:]
    half = jnp.where(iota((16, lanes), 0) < 8, 0.0, 1.0).astype(BF)
    one = jnp.ones((16, lanes), BF)
    zero = jnp.zeros((16, lanes), BF)

    edge = (lane < 4) | (lane >= lanes - 4)

    def slope(z, t):
        row = 8 + 8 * t
        tile = xe[4 + z, pl.ds(row, 8), :]
        rx, ry, rz = None, None, None
        for k, c in enumerate(RATIO, start=1):
            dz = xe[4 + z + k, pl.ds(row, 8), :] - xe[4 + z - k, pl.ds(row, 8), :]
            dy = xe[4 + z, pl.ds(row + k, 8), :] - xe[4 + z, pl.ds(row - k, 8), :]
            dx = pltpu.roll(tile, lanes - k, 1) - pltpu.roll(tile, k, 1)
            rz = dz if rz is None else rz + c * dz
            ry = dy if ry is None else ry + c * dy
            rx = dx if rx is None else rx + c * dx
        return rz * rz + ry * ry, rx

    def cell(square, state, masked):
        total, number, most, least = state
        square = square * (COEF[0] * COEF[0]) + 1.0
        m = square * lax.rsqrt(square) - 1.0
        q = jnp.minimum(jnp.maximum(m * (BINS / RANGE) - 0.5, 0.0), BINS - 1.0)
        if masked:
            q = jnp.where(edge, -64.0, q)
        low = jnp.floor(q)
        frac = q - low
        weight = jnp.maximum(jnp.minimum(jnp.minimum(q - lower, 1.0), upper - q), 0.0)
        wm = weight * m
        under = m - RANGE * weight
        if masked:
            under = jnp.where(edge, jnp.inf, under)
        state = total + wm, number + weight, jnp.maximum(most, wm), jnp.minimum(least, under)
        coarse = jnp.floor((low + 0.5) * (1.0 / FINE))
        fine = low - FINE * coarse
        th = twice(frac)
        tl = twice(frac - th[:8].astype(F32))
        c2 = twice(coarse) - half
        f2 = twice(fine) - half
        here = [f2 == 2.0 * i for i in range(FINE // 2)]
        left = jnp.concatenate([jnp.where(c2 == 2.0 * i, one, zero) for i in range(COARSE // 2)], axis=0)
        right = jnp.concatenate([jnp.where(h, v, zero) for v in (one, th, tl) for h in here], axis=0)
        return m, state, left, right

    def gather(pairs):
        product = None
        for at in range(0, len(pairs), 8):
            left, right = zip(*pairs[at:at + 8])
            dot = lax.dot_general(
                jnp.concatenate(left, axis=1), jnp.concatenate(right, axis=1),
                (((1,), (1,)), ((), ())), preferred_element_type=F32)
            product = dot if product is None else product + dot
        acc[...] += product

    def body(places, state, chosen, fresh):
        pairs = []
        for z, odd in places:
            if not odd:
                flats = jnp.zeros((8, lanes), F32) if fresh else flat[z // 2]
                bends = jnp.zeros((8, lanes), F32) if fresh else bend[z // 2]
            for t in chosen:
                g = 8 * odd + t
                square, rx = slope(z, t)
                flats = jnp.where(group == g, pltpu.roll(square, (4 + 8 * g) % lanes, 1), flats)
                bends = jnp.where(group == g, pltpu.roll(rx, (4 + 8 * g) % lanes, 1), bends)
                m, state, left, right = cell(square + rx * rx, state, True)
                mag[z, pl.ds(8 * t, 8), :] = m
                pairs.append((left, right))
            if odd:
                flat[z // 2] = flats
                bend[z // 2] = bends
        return pairs, state

    inner = range(1, tiles - 1)
    outer = (0, tiles - 1)

    def middle(turn, state):
        @pl.when(turn == 1)
        def _():
            pl.semaphore_wait(known.at[0], len(near))
            tell(known.at[1], [away(axis, d) for axis in ("gy", "gz") for d in (2, -2)])

        pairs, state = body([(4 + planes * turn + i, i % 2) for i in range(planes)], state, inner, True)
        gather(pairs)
        return state

    start = jnp.zeros((8, lanes), F32)
    state = (start, start, start - jnp.inf, start + jnp.inf)
    planes = (zs - 8) // 2
    state = lax.fori_loop(0, 2, middle, state)
    pl.semaphore_wait(known.at[1], 4)
    tell(known.at[2], [away("gy", 4), away("gy", -4)] + [away("gx", d) for d in range(1, nx)])
    for copy in rows_y + depths + rows_x:
        copy.wait()
    lax.fori_loop(0, zs // 2, unpack_y, 0)

    pairs, state = body([(z, z % 2) for z in range(4, zs - 4)], state, outer, False)
    more, state = body([(z, z % 2) for z in range(zs) if z < 4 or z >= zs - 4], state, range(tiles), True)
    pairs = pairs + more
    for p in range(zs // 2):
        west, east = xl[p % quarter], xr[p % quarter]
        if p >= quarter:
            west, east = pltpu.roll(west, lanes - 4, 1), pltpu.roll(east, 4, 1)
        e = jnp.where(part < 4, west, east) - xp[p]
        high = jnp.where(part >= 4, e, 0.0)
        low = jnp.where(part < 4, e, 0.0)
        ahead, behind = 0.0, 0.0
        for k, c in enumerate(RATIO, start=1):
            ahead = ahead + c * pltpu.roll(high, lanes - k, 1)
            behind = behind + c * pltpu.roll(low, k, 1)
        rx = bend[p] + jnp.where(part < 4, ahead, -behind)
        m, state, left, right = cell(flat[p] + rx * rx, state, False)
        rim[p] = m
        pairs.append((left, right))
    gather(pairs)
    total, number, most, least = state

    def mend(p, carry):
        for g in range(16):
            place = (2 * p + g // 8, pl.ds(8 * (g % 8), 8))
            mag[place] = jnp.where(edge, pltpu.roll(rim[p], (lanes - 4 - 8 * g) % lanes, 1), mag[place])
        return carry

    prod = jnp.where(iota((ROWS, COLS), 0) % 8 == iota((ROWS, COLS), 1) % 8, acc[...], 0.0)
    table = jnp.sum(prod.reshape(COARSE, 8, COLS), axis=1)
    one_part = table.astype(BF)
    rest = table - one_part.astype(F32)
    two_part = rest.astype(BF)
    three_part = (rest - two_part.astype(F32)).astype(BF)
    crow = iota((COARSE, BINS), 0)
    cbin = iota((COARSE, BINS), 1)

    def spread(v):
        return lax.dot_general(v, pick[...], (((1,), (0,)), ((), ())), preferred_element_type=F32)

    wide = spread(one_part) + spread(two_part) + spread(three_part)
    counts = jnp.sum(
        jnp.where(crow == cbin // FINE, wide[:, :BINS], 0.0)
        + jnp.where(crow + 1 == (cbin + FINE - 1) // FINE, wide[:, BINS:], 0.0),
        axis=0, keepdims=True)
    r4, l4 = iota((3, 128), 0), iota((3, 128), 1)
    mine = jnp.where(r4 == 0, counts[:, :128], jnp.where(r4 == 1, counts[:, 128:], 0.0))
    for i, v in enumerate((-RANGE - jnp.min(least), jnp.max(most), jnp.sum(total), jnp.sum(number))):
        mine = jnp.where((r4 == 2) & (l4 == i), v, mine)
    is_max = (r4 == 2) & (l4 < 2)

    def exchange(value, own, buffer, place, peers, sems, work=None):
        own[...] = value
        buffer[place] = value
        for peer in peers:
            pltpu.make_async_remote_copy(
                src_ref=own, dst_ref=buffer.at[place], send_sem=sems.at[0], recv_sem=sems.at[1],
                device_id=peer, device_id_type=MESH).start()
        if work is not None:
            work()
        every = buffer.at[pl.ds(0, len(peers))]
        pltpu.make_async_copy(every, every, sems.at[1]).wait()
        added, top = buffer[0], buffer[0]
        for i in range(1, buffer.shape[0]):
            added = added + buffer[i]
            top = jnp.maximum(top, buffer[i])
        return jnp.where(is_max, top, added)

    pl.semaphore_wait(known.at[2], nx + 1)
    mine = exchange(mine, own.at[0], plane, gx * nz + gz,
                    [away("gx", dx) | away("gz", dz) for dx in (2, 1, 3, 0) for dz in (2, 6, 5, 3, 4, 1, 7, 0) if dx or dz],
                    plane_sem, lambda: lax.fori_loop(0, zs // 2, mend, 0))
    mine = exchange(mine, own.at[1], line, gy, [away("gy", d) for d in (8, 7, 9, 6, 10, 5, 11, 4, 12, 3, 13, 2, 14, 1, 15)], line_sem)

    hist[...] = mine[:2] * (BINS / cells)
    last, l1 = mine[2:, :4], iota((1, 4), 1)
    for buffer, sems in ((plane, plane_sem), (line, line_sem)):
        sent = buffer.at[pl.ds(0, buffer.shape[0] - 1)]
        pltpu.make_async_copy(sent, sent, sems.at[0]).wait()
    stat[...] = jnp.where(l1 == 0, -last, jnp.where(l1 == 1, last, last / cells))


def finish(mag, hist, stat, mag_ref, hist_ref, stat_ref, sems):
    copies = [
        pltpu.make_async_copy(source, target, sems.at[i])
        for i, (source, target) in enumerate(((mag, mag_ref), (hist, hist_ref), (stat, stat_ref)))
    ]
    for copy in copies:
        copy.start()
    for copy in copies:
        copy.wait()


def solution(mesh):
    nx, ny, nz = mesh.shape["gx"], mesh.shape["gy"], mesh.shape["gz"]

    def on_device(x, first, beyond):
        zs, ys, xs = x.shape
        cells = float(zs * ys * xs * nx * ny * nz)
        vmem = pl.BlockSpec(memory_space=pltpu.VMEM)
        hbm = pl.BlockSpec(memory_space=pltpu.HBM)
        dma = pltpu.SemaphoreType.DMA
        window = jnp.concatenate([jnp.broadcast_to(v.astype(F32), (1, xs)) for v in (first, beyond)])
        window = pltpu.with_memory_space_constraint(window, pltpu.VMEM)
        packed = pltpu.VMEM((zs // 2, 8, xs), F32)
        slim = pltpu.VMEM((zs // 4, 8, xs), F32)
        parts = pl.pallas_call(
            lambda *refs: kernel(nx, ny, nz, cells, *refs),
            name="field",
            out_shape=(pltpu.VMEM(x.shape, F32), pltpu.VMEM((2, 128), F32), pltpu.VMEM((1, 4), F32)),
            in_specs=[vmem, hbm],
            out_specs=(vmem, vmem, vmem),
            scratch_shapes=[
                pltpu.VMEM((zs + 8, ys + 16, xs), F32),
                packed, slim, slim, slim, slim,
                packed, packed, packed, packed,
                packed, packed, packed,
                pltpu.VMEM((COLS, 2 * BINS), BF),
                pltpu.VMEM((ROWS, COLS), F32),
                pltpu.VMEM((2, 3, 128), F32),
                pltpu.VMEM((nx * nz, 3, 128), F32),
                pltpu.VMEM((ny, 3, 128), F32),
                dma, dma((6,)), dma((6,)), dma((2,)), dma((2,)),
                pltpu.SemaphoreType.REGULAR((3,)),
            ],
            compiler_params=pltpu.CompilerParams(collective_id=0, has_side_effects=True),
        )(window, x)
        parts = [pltpu.with_memory_space_constraint(v, pltpu.VMEM) for v in parts]
        mag, hist, stat = pl.pallas_call(
            finish,
            name="finish",
            out_shape=tuple(jax.ShapeDtypeStruct(v.shape, F32) for v in parts),
            in_specs=[vmem, vmem, vmem],
            out_specs=(hbm, hbm, hbm),
            scratch_shapes=[dma((3,))],
        )(*parts)
        return mag, hist.reshape(BINS), stat.reshape(4)

    return jax.shard_map(
        on_device, mesh=mesh,
        in_specs=(P("gz", "gy", "gx"), P(), P()),
        out_specs=(P("gz", "gy", "gx"), P(), P()),
        check_vma=False,
    )
```

```python
import jax
import jax.numpy as jnp
from jax import lax
from jax.experimental import pallas as pl
from jax.experimental.pallas import tpu as pltpu
from jax.sharding import PartitionSpec as P

BINS = 256
RANGE = 12.0
COEF = (0.8, -0.2, 4.0 / 105.0, -1.0 / 280.0)
RATIO = tuple(c / COEF[0] for c in COEF)
FINE = 10
COARSE = 26
ROWS, COLS = 8 * COARSE, 24 * FINE
ROUND = 49152.0
MESH = pl.DeviceIdType.MESH
BF = jnp.bfloat16
F32 = jnp.float32


def iota(shape, dim):
    return lax.broadcasted_iota(jnp.int32, shape, dim)


def twice(v):
    return jnp.concatenate([v, v], axis=0).astype(BF)


def kernel(nx, ny, nz, cells, window, x_ref, mag, hist, stat,
           xe, xp, xh, xw, xl, xr, yph, ypl, yrh, yrl, flat, bend, rim, pick, acc, own, plane, line,
           in_sem, halo_send, halo_recv, plane_sem, line_sem, known):
    gx, gy, gz = lax.axis_index("gx"), lax.axis_index("gy"), lax.axis_index("gz")
    zs, ys, lanes = x_ref.shape
    tiles = ys // 8

    def away(axis, d):
        here, size = {"gx": (gx, nx), "gy": (gy, ny), "gz": (gz, nz)}[axis]
        return {axis: lax.rem(here + d % size, size)}

    def tell(sem, peers):
        for peer in peers:
            pl.semaphore_signal(sem, inc=1, device_id=peer, device_id_type=MESH)

    near = [away(axis, d) for axis in ("gx", "gy", "gz") for d in (1, -1)]
    barrier = pltpu.get_barrier_semaphore()
    load = pltpu.make_async_copy(x_ref, xe.at[pl.ds(4, zs), pl.ds(8, ys), :], in_sem)
    for z in range(0, zs, 4):
        pltpu.make_async_copy(
            x_ref.at[pl.ds(z, 4)], xe.at[pl.ds(4 + z, 4), pl.ds(8, ys), :], in_sem).start()
    tell(barrier, near)

    lane = iota((8, lanes), 1)
    sub = iota((8, lanes), 0)
    group, part = lane // 8, lane % 8
    acc[...] = jnp.zeros_like(acc)
    kind, digit = iota((COLS, BINS), 0) // (8 * FINE), (iota((COLS, BINS), 0) // 8) % FINE
    bin_ = iota((COLS, BINS), 1)
    picked = jnp.where(digit == bin_ % FINE, jnp.where(kind == 0, 1.0, -1.0), 0.0)
    moved = jnp.where((digit == (bin_ + FINE - 1) % FINE) & (kind > 0), 1.0, 0.0)
    pick[:, :BINS] = picked.astype(BF)
    pick[:, BINS:] = moved.astype(BF)

    load.wait()

    def pack_y(i, carry):
        z = 4 + 2 * i
        yph[i] = jnp.where(sub < 4, xe[z, pl.ds(ys + 4, 8), :], xe[z + 1, pl.ds(ys, 8), :])
        ypl[i] = jnp.where(sub < 4, xe[z, pl.ds(8, 8), :], xe[z + 1, pl.ds(4, 8), :])
        return carry

    lax.fori_loop(0, zs // 2, pack_y, 0)
    for p in range(zs // 2):
        packed = jnp.zeros((8, lanes), F32)
        for g in range(16):
            tile = xe[4 + 2 * p + g // 8, pl.ds(8 + 8 * (g % 8), 8), :]
            packed = jnp.where(group == g, pltpu.roll(tile, (4 + 8 * g) % lanes, 1), packed)
        xp[p] = packed
    quarter = zs // 4
    for p in range(quarter):
        near_p, far_p = xp[p], xp[p + quarter]
        xh[p] = jnp.where(part < 4, near_p, pltpu.roll(far_p, 4, 1))
        xw[p] = jnp.where(part >= 4, near_p, pltpu.roll(far_p, lanes - 4, 1))
    pl.semaphore_wait(barrier, len(near))

    def send(i, src, dst, peer):
        copy = pltpu.make_async_remote_copy(
            src_ref=src, dst_ref=dst, send_sem=halo_send.at[i], recv_sem=halo_recv.at[i],
            device_id=peer, device_id_type=MESH)
        copy.start()
        return copy

    mid_y = pl.ds(8, ys)
    rows_x = [
        send(0, xh, xl, away("gx", 1)),
        send(1, xw, xr, away("gx", -1)),
    ]
    rows_y = [
        send(2, yph, yrh, away("gy", 1)),
        send(3, ypl, yrl, away("gy", -1)),
    ]
    depths = [
        send(4, xe.at[pl.ds(zs, 4), mid_y, :], xe.at[pl.ds(0, 4), mid_y, :], away("gz", 1)),
        send(5, xe.at[pl.ds(4, 4), mid_y, :], xe.at[pl.ds(zs + 4, 4), mid_y, :], away("gz", -1)),
    ]
    tell(known.at[0], near)

    def unpack_y(i, carry):
        z = 4 + 2 * i
        below, above = yrh[i], yrl[i]
        xe[z, pl.ds(4, 4), :] = below[:4]
        xe[z + 1, pl.ds(4, 4), :] = below[4:]
        xe[z, pl.ds(ys + 8, 4), :] = above[:4]
        xe[z + 1, pl.ds(ys + 8, 4), :] = above[4:]
        return carry

    lower, upper = window[:1] - 1.0, window[1:]
    half = jnp.where(iota((16, lanes), 0) < 8, 0.0, 1.0).astype(BF)
    one = jnp.ones((16, lanes), BF)
    zero = jnp.zeros((16, lanes), BF)

    edge = (lane < 4) | (lane >= lanes - 4)

    def slope(z, t):
        row = 8 + 8 * t
        tile = xe[4 + z, pl.ds(row, 8), :]
        rx, ry, rz = None, None, None
        for k, c in enumerate(RATIO, start=1):
            dz = xe[4 + z + k, pl.ds(row, 8), :] - xe[4 + z - k, pl.ds(row, 8), :]
            dy = xe[4 + z, pl.ds(row + k, 8), :] - xe[4 + z, pl.ds(row - k, 8), :]
            dx = pltpu.roll(tile, lanes - k, 1) - pltpu.roll(tile, k, 1)
            rz = dz if rz is None else rz + c * dz
            ry = dy if ry is None else ry + c * dy
            rx = dx if rx is None else rx + c * dx
        return rz * rz + ry * ry, rx

    def cell(square, state, masked):
        total, number, most, least = state
        square = square * (COEF[0] * COEF[0]) + 1.0
        m = square * lax.rsqrt(square) - 1.0
        q = jnp.minimum(jnp.maximum(m * (BINS / RANGE) - 0.5, 0.0), BINS - 1.0)
        if masked:
            q = jnp.where(edge, -64.0, q)
        low = jnp.floor(q)
        frac = q - low
        weight = jnp.maximum(jnp.minimum(jnp.minimum(q - lower, 1.0), upper - q), 0.0)
        wm = weight * m
        under = m - RANGE * weight
        if masked:
            under = jnp.where(edge, jnp.inf, under)
        state = total + wm, number + weight, jnp.maximum(most, wm), jnp.minimum(least, under)
        coarse = jnp.floor((low + 0.5) * (1.0 / FINE))
        fine = low - FINE * coarse
        th = twice(frac)
        tl = twice(frac - th[:8].astype(F32))
        c2 = twice(coarse) - half
        f2 = twice(fine) - half
        here = [f2 == 2.0 * i for i in range(FINE // 2)]
        left = jnp.concatenate([jnp.where(c2 == 2.0 * i, one, zero) for i in range(COARSE // 2)], axis=0)
        right = jnp.concatenate([jnp.where(h, v, zero) for v in (one, th, tl) for h in here], axis=0)
        return m, state, left, right

    def gather(pairs):
        product = None
        for at in range(0, len(pairs), 8):
            left, right = zip(*pairs[at:at + 8])
            dot = lax.dot_general(
                jnp.concatenate(left, axis=1), jnp.concatenate(right, axis=1),
                (((1,), (1,)), ((), ())), preferred_element_type=F32)
            product = dot if product is None else product + dot
        acc[...] += product

    def body(places, state, chosen, fresh):
        pairs = []
        for z, odd in places:
            if not odd:
                flats = jnp.zeros((8, lanes), F32) if fresh else flat[z // 2]
                bends = jnp.zeros((8, lanes), F32) if fresh else bend[z // 2]
            for t in chosen:
                g = 8 * odd + t
                square, rx = slope(z, t)
                flats = jnp.where(group == g, pltpu.roll(square, (4 + 8 * g) % lanes, 1), flats)
                bends = jnp.where(group == g, pltpu.roll(rx, (4 + 8 * g) % lanes, 1), bends)
                m, state, left, right = cell(square + rx * rx, state, True)
                mag[z, pl.ds(8 * t, 8), :] = m
                pairs.append((left, right))
            if odd:
                flat[z // 2] = flats
                bend[z // 2] = bends
        return pairs, state

    inner = range(1, tiles - 1)
    outer = (0, tiles - 1)

    def middle(turn, state):
        @pl.when(turn == 1)
        def _():
            pl.semaphore_wait(known.at[0], len(near))
            tell(known.at[1], [away(axis, d) for axis in ("gy", "gz") for d in (2, -2)])

        pairs, state = body([(4 + planes * turn + i, i % 2) for i in range(planes)], state, inner, True)
        gather(pairs)
        return state

    start = jnp.zeros((8, lanes), F32)
    state = (start, start, start - jnp.inf, start + jnp.inf)
    planes = (zs - 8) // 2
    state = lax.fori_loop(0, 2, middle, state)
    pl.semaphore_wait(known.at[1], 4)
    tell(known.at[2], [away("gy", 4), away("gy", -4)] + [away("gx", d) for d in range(1, nx)])
    for copy in rows_y + depths + rows_x:
        copy.wait()
    lax.fori_loop(0, zs // 2, unpack_y, 0)

    pairs, state = body([(z, z % 2) for z in range(4, zs - 4)], state, outer, False)
    more, state = body([(z, z % 2) for z in range(zs) if z < 4 or z >= zs - 4], state, range(tiles), True)
    pairs = pairs + more
    for p in range(zs // 2):
        west, east = xl[p % quarter], xr[p % quarter]
        if p >= quarter:
            west, east = pltpu.roll(west, lanes - 4, 1), pltpu.roll(east, 4, 1)
        e = jnp.where(part < 4, west, east) - xp[p]
        high = jnp.where(part >= 4, e, 0.0)
        low = jnp.where(part < 4, e, 0.0)
        ahead, behind = 0.0, 0.0
        for k, c in enumerate(RATIO, start=1):
            ahead = ahead + c * pltpu.roll(high, lanes - k, 1)
            behind = behind + c * pltpu.roll(low, k, 1)
        rx = bend[p] + jnp.where(part < 4, ahead, -behind)
        m, state, left, right = cell(flat[p] + rx * rx, state, False)
        rim[p] = m
        pairs.append((left, right))
    gather(pairs)
    total, number, most, least = state

    def mend(p, carry):
        for g in range(16):
            place = (2 * p + g // 8, pl.ds(8 * (g % 8), 8))
            mag[place] = jnp.where(edge, pltpu.roll(rim[p], (lanes - 4 - 8 * g) % lanes, 1), mag[place])
        return carry

    prod = jnp.where(iota((ROWS, COLS), 0) % 8 == iota((ROWS, COLS), 1) % 8, acc[...], 0.0)
    table = jnp.sum(prod.reshape(COARSE, 8, COLS), axis=1)
    one_part = table.astype(BF)
    rest = table - one_part.astype(F32)
    two_part = rest.astype(BF)
    three_part = (rest - two_part.astype(F32)).astype(BF)
    crow = iota((COARSE, BINS), 0)
    cbin = iota((COARSE, BINS), 1)

    def spread(v):
        return lax.dot_general(v, pick[...], (((1,), (0,)), ((), ())), preferred_element_type=F32)

    wide = spread(one_part) + spread(two_part) + spread(three_part)
    counts = jnp.sum(
        jnp.where(crow == cbin // FINE, wide[:, :BINS], 0.0)
        + jnp.where(crow + 1 == (cbin + FINE - 1) // FINE, wide[:, BINS:], 0.0),
        axis=0, keepdims=True)
    r4, l4 = iota((3, 128), 0), iota((3, 128), 1)
    mine = jnp.where(r4 == 0, counts[:, :128], jnp.where(r4 == 1, counts[:, 128:], 0.0))
    for i, v in enumerate((-RANGE - jnp.min(least), jnp.max(most), jnp.sum(total), jnp.sum(number))):
        mine = jnp.where((r4 == 2) & (l4 == i), v, mine)
    is_max = (r4 == 2) & (l4 < 2)

    def exchange(value, own, buffer, place, peers, sems, work=None):
        own[...] = value
        buffer[place] = value
        for peer in peers:
            pltpu.make_async_remote_copy(
                src_ref=own, dst_ref=buffer.at[place], send_sem=sems.at[0], recv_sem=sems.at[1],
                device_id=peer, device_id_type=MESH).start()
        if work is not None:
            work()
        every = buffer.at[pl.ds(0, len(peers))]
        pltpu.make_async_copy(every, every, sems.at[1]).wait()
        added, top = buffer[0], buffer[0]
        for i in range(1, buffer.shape[0]):
            added = added + buffer[i]
            top = jnp.maximum(top, buffer[i])
        return jnp.where(is_max, top, added)

    pl.semaphore_wait(known.at[2], nx + 1)
    mine = exchange(mine, own.at[0], plane, gx * nz + gz,
                    [away("gx", dx) | away("gz", dz) for dx in (2, 1, 3, 0) for dz in (2, 6, 5, 3, 4, 1, 7, 0) if dx or dz],
                    plane_sem, lambda: lax.fori_loop(0, zs // 2, mend, 0))
    mine = exchange(mine, own.at[1], line, gy, [away("gy", d) for d in (8, 7, 9, 6, 10, 5, 11, 4, 12, 3, 13, 2, 14, 1, 15)], line_sem)

    hist[...] = mine[:2] * (BINS / cells)
    last, l1 = mine[2:, :4], iota((1, 4), 1)
    for buffer, sems in ((plane, plane_sem), (line, line_sem)):
        sent = buffer.at[pl.ds(0, buffer.shape[0] - 1)]
        pltpu.make_async_copy(sent, sent, sems.at[0]).wait()
    stat[...] = jnp.where(l1 == 0, -last, jnp.where(l1 == 1, last, last / cells))


def finish(mag, hist, stat, mag_ref, hist_ref, stat_ref, sems):
    copies = [
        pltpu.make_async_copy(source, target, sems.at[i])
        for i, (source, target) in enumerate(((mag, mag_ref), (hist, hist_ref), (stat, stat_ref)))
    ]
    for copy in copies:
        copy.start()
    for copy in copies:
        copy.wait()


def solution(mesh):
    nx, ny, nz = mesh.shape["gx"], mesh.shape["gy"], mesh.shape["gz"]

    def on_device(x, first, beyond):
        zs, ys, xs = x.shape
        cells = float(zs * ys * xs * nx * ny * nz)
        vmem = pl.BlockSpec(memory_space=pltpu.VMEM)
        hbm = pl.BlockSpec(memory_space=pltpu.HBM)
        dma = pltpu.SemaphoreType.DMA
        window = jnp.concatenate([jnp.broadcast_to(v.astype(F32), (1, xs)) for v in (first, beyond)])
        window = pltpu.with_memory_space_constraint(window, pltpu.VMEM)
        packed = pltpu.VMEM((zs // 2, 8, xs), F32)
        slim = pltpu.VMEM((zs // 4, 8, xs), F32)
        parts = pl.pallas_call(
            lambda *refs: kernel(nx, ny, nz, cells, *refs),
            name="field",
            out_shape=(pltpu.VMEM(x.shape, F32), pltpu.VMEM((2, 128), F32), pltpu.VMEM((1, 4), F32)),
            in_specs=[vmem, hbm],
            out_specs=(vmem, vmem, vmem),
            scratch_shapes=[
                pltpu.VMEM((zs + 8, ys + 16, xs), F32),
                packed, slim, slim, slim, slim,
                packed, packed, packed, packed,
                packed, packed, packed,
                pltpu.VMEM((COLS, 2 * BINS), BF),
                pltpu.VMEM((ROWS, COLS), F32),
                pltpu.VMEM((2, 3, 128), F32),
                pltpu.VMEM((nx * nz, 3, 128), F32),
                pltpu.VMEM((ny, 3, 128), F32),
                dma, dma((6,)), dma((6,)), dma((2,)), dma((2,)),
                pltpu.SemaphoreType.REGULAR((3,)),
            ],
            compiler_params=pltpu.CompilerParams(collective_id=0, has_side_effects=True),
        )(window, x)
        parts = [pltpu.with_memory_space_constraint(v, pltpu.VMEM) for v in parts]
        mag, hist, stat = pl.pallas_call(
            finish,
            name="finish",
            out_shape=tuple(jax.ShapeDtypeStruct(v.shape, F32) for v in parts),
            in_specs=[vmem, vmem, vmem],
            out_specs=(hbm, hbm, hbm),
            scratch_shapes=[dma((3,))],
        )(*parts)
        return mag, hist.reshape(BINS), stat.reshape(4)

    return jax.shard_map(
        on_device, mesh=mesh,
        in_specs=(P("gz", "gy", "gx"), P(), P()),
        out_specs=(P("gz", "gy", "gx"), P(), P()),
        check_vma=False,
    )
```
